16 devices in a mesh: tasks: 2 (over y, z), group: 8 (over x, core).
Axes of the slice: x: 4, y: 2, z: 1, core: 2. Of those that a mesh axis runs over, the one named last changes fastest.
The devices are a block of a 4x4x8 slice.
Arguments:
- points: bfloat16 [32768, 384], P(('tasks', 'group')), parts along dimension 0
- vectors: bfloat16 [32768, 64], P(('tasks', 'group')), parts along dimension 0
- lengthscale: float32 [1], replicated
- outscale: float32 [1], replicated
Outputs:
- output: float32 [32768, 64], P(('tasks', 'group')), parts along dimension 0
There are 2 independent parts. The reference program is written for one: setup_inputs(seed, part) draws one part's arguments, and reference() takes and returns one part's arrays. A program takes and returns all parts, laid end to end along the dimension named above; an argument that names none is the same for every part.
All inputs are finite; a program needn't handle non-finite values.
Results may differ from the reference program's by a relative error of at most 0.001.
Values are sent between devices in bfloat16 or wider.
A program may use at most 768 MiB of HBM per device.

```python
import jax
import jax.numpy as jnp
from jax import lax

NUM_POINTS = 16384
FEAT_DIM = 384
NUM_RHS = 64
QUERY_BLOCK = 256
LATENT_DIM = 8


def setup_inputs(seed: int = 0, part: int = 0) -> dict:
    base_key = jax.random.key(seed)
    part_key = jax.random.fold_in(base_key, part)
    key_lat, key_mix, key_noise, key_rhs = jax.random.split(part_key, 4)
    key_ell, key_scale = jax.random.split(jax.random.key(seed + 29), 2)
    latent = jax.random.normal(key_lat, (NUM_POINTS, LATENT_DIM), jnp.float32)
    mixing = jax.random.normal(key_mix, (LATENT_DIM, FEAT_DIM), jnp.float32) * FEAT_DIM ** -0.5
    noise = jax.random.normal(key_noise, (NUM_POINTS, FEAT_DIM), jnp.float32) * (0.3 * FEAT_DIM ** -0.5)
    points = (jnp.dot(latent, mixing) + noise).astype(jnp.bfloat16)
    vectors = (jax.random.normal(key_rhs, (NUM_POINTS, NUM_RHS), jnp.float32) * NUM_POINTS ** -0.5).astype(jnp.bfloat16)
    lengthscale = jax.random.uniform(key_ell, (1,), jnp.float32, 2.4, 3.1)
    outscale = jax.random.uniform(key_scale, (1,), jnp.float32, 0.6, 1.6)
    return {'points': points, 'vectors': vectors, 'lengthscale': lengthscale, 'outscale': outscale}


def reference(points, vectors, lengthscale, outscale):
    sq_norm = jnp.sum(jnp.square(points.astype(jnp.float32)), axis=1)
    two_ell_sq = 2.0 * jnp.square(lengthscale[0])
    query_pts = points.reshape(NUM_POINTS // QUERY_BLOCK, QUERY_BLOCK, FEAT_DIM)
    query_norm = sq_norm.reshape(NUM_POINTS // QUERY_BLOCK, QUERY_BLOCK)

    def one_block(block_pair):
        block_pts, block_norm = block_pair
        gram_mat = jnp.dot(block_pts, points.T, preferred_element_type=jnp.float32)
        sq_dist = jnp.maximum(block_norm[:, None] + sq_norm[None, :] - 2.0 * gram_mat, 0.0)
        kern_blk = (outscale[0] * jnp.exp(-sq_dist / two_ell_sq)).astype(jnp.bfloat16)
        return jnp.dot(kern_blk, vectors, preferred_element_type=jnp.float32)

    result = lax.map(one_block, (query_pts, query_norm))
    return result.reshape(NUM_POINTS, NUM_RHS)
```

```python
import functools

import jax
import jax.numpy as jnp
from jax import lax
from jax.experimental import pallas as pl
from jax.experimental.pallas import tpu as pltpu
from jax.sharding import PartitionSpec as P

CH = 256
LOG2E = 1.4426950408889634
OWN, SIB, LFT, RGT, LFT2, RGT2 = 0, 8, 16, 24, 32, 40
N_STEPS = 32


def ext_values(x):
    xf = x.astype(jnp.float32)
    h = -0.5 * jnp.sum(xf * xf, axis=1, keepdims=True)
    hi = h.astype(jnp.bfloat16).astype(jnp.float32)
    r = jnp.where(h == hi, 0.0, h - hi)
    mid = r.astype(jnp.bfloat16).astype(jnp.float32)
    return hi, mid, r - mid


def ext_rows(x, first):
    hi, mid, lo = ext_values(x)
    lane = lax.broadcasted_iota(jnp.int32, (x.shape[0], 128), 1)
    e = jnp.where(lane < 6, 1.0, 0.0)
    e = jnp.where(lane == first, hi, e)
    e = jnp.where(lane == first + 1, mid, e)
    e = jnp.where(lane == first + 2, lo, e)
    return e.astype(jnp.bfloat16)


def describe(t):
    w = jnp.where
    early = t < 8
    mid = (t >= 8) & (t < 16)
    u = jnp.maximum(t - 19, 0)
    is_new_far = (t >= 19) & (t <= 28) & (lax.rem(u, 3) == 0)
    m = t - 16 - w(t >= 20, jnp.minimum((jnp.maximum(t - 20, 0)) // 3 + 1, 4), 0)
    is_far = (t >= 16) & (is_new_far | (m < 4))
    q = w(mid, (t - 8) // 2, w(is_new_far, 4 + u // 3, w(m < 4, m, 4 + (m - 4) // 2)))
    second = w(mid, lax.rem(t, 2), lax.rem(jnp.maximum(m, 0), 2)) == 1
    q = w(early, 0, q)
    own_a = w(early, 2 * t, w(second, LFT2, LFT) + q)
    own_b = w(early, 2 * t + 1, w(second, RGT2, RGT) + q)
    a0 = w(is_far, LFT + q, own_a)
    b0 = w(is_far, LFT2 + q, own_b)
    a1 = w(is_far, RGT + q, own_a)
    b1 = w(is_far, RGT2 + q, own_b)
    return a0, b0, a1, b1, w(is_far, 8, 0)


def kernel(n, x_hbm, vt_hbm, sc_ref, out_ref,
           xb, vb, xe, xr, ka, kb, y, part, pin,
           loc_sem, sx, sv, rx, rv, ps, pr):
    me = lax.axis_index("group")
    core = lax.rem(me, 2)
    sib = me + 1 - 2 * core
    left = lax.rem(me + n - 2, n)
    right = lax.rem(me + 2, n)

    def remote(src, dst, ssem, rsem, dev):
        return pltpu.make_async_remote_copy(
            src_ref=src, dst_ref=dst, send_sem=ssem, recv_sem=rsem,
            device_id={"group": dev}, device_id_type=pl.DeviceIdType.MESH)

    own_x = pltpu.make_async_copy(x_hbm, xb.at[pl.ds(OWN, 8)], loc_sem.at[0])
    own_v = pltpu.make_async_copy(vt_hbm, vb.at[pl.ds(OWN, 8)], loc_sem.at[1])
    own_x.start()
    own_v.start()
    barrier = pltpu.get_barrier_semaphore()
    for dev in (sib, left, right):
        pl.semaphore_signal(barrier, inc=1, device_id={"group": dev},
                            device_id_type=pl.DeviceIdType.MESH)
    own_x.wait()
    own_v.wait()
    pl.semaphore_wait(barrier, 3)

    def to_left(q, o):
        return (remote(xb.at[OWN + o], xb.at[LFT + q], sx.at[q], rx.at[LFT + q], left),
                remote(vb.at[OWN + o], vb.at[LFT + q], sv.at[q], rv.at[LFT + q], left))

    def to_right(q, o):
        return (remote(xb.at[OWN + o], xb.at[RGT + q], sx.at[8 + q], rx.at[RGT + q], right),
                remote(vb.at[OWN + o], vb.at[RGT + q], sv.at[8 + q], rv.at[RGT + q], right))

    def to_sib():
        return (remote(xb.at[pl.ds(OWN, 8)], xb.at[pl.ds(SIB, 8)], sx.at[16], rx.at[SIB], sib),
                remote(vb.at[pl.ds(OWN, 8)], vb.at[pl.ds(SIB, 8)], sv.at[16], rv.at[SIB], sib))

    def fwd(q):
        return (remote(xb.at[LFT + q], xb.at[LFT2 + q], sx.at[17 + q], rx.at[LFT2 + q], sib),
                remote(vb.at[LFT + q], vb.at[LFT2 + q], sv.at[17 + q], rv.at[LFT2 + q], sib),
                remote(xb.at[RGT + q], xb.at[RGT2 + q], sx.at[25 + q], rx.at[RGT2 + q], sib),
                remote(vb.at[RGT + q], vb.at[RGT2 + q], sv.at[25 + q], rv.at[RGT2 + q], sib))

    def partial_copies():
        return (remote(part.at[pl.ds(0, 4)], pin.at[pl.ds(0, 4)], ps.at[0], pr.at[0], left),
                remote(part.at[pl.ds(4, 4)], pin.at[pl.ds(4, 4)], ps.at[1], pr.at[1], right))

    for q in range(8):
        for c in to_left(q, (q + 4) % 8) + to_right(q, q):
            c.start()
        if q == 0:
            for c in to_sib():
                c.start()

    two_ell_sq = 2.0 * sc_ref[0] * sc_ref[0]

    def target(slot, tile):
        xv = xb[slot]
        full = jnp.concatenate([xv, ext_rows(xv, 3)], axis=1)
        xr[tile] = full.T

    lax.fori_loop(0, 8, lambda i, _: (target(OWN + i, i), 0)[1], 0)
    y[...] = jnp.zeros_like(y)
    kb[...] = jnp.zeros_like(kb)

    c2 = sc_ref[2]
    ls = sc_ref[3]

    def gram(d, dst):
        a0, b0, a1, b1, tb = d
        for g, (a, b) in enumerate(((a0, b0), (a1, b1))):
            lhs = jnp.concatenate(
                [jnp.concatenate([xb[a], xe[a]], axis=1),
                 jnp.concatenate([xb[b], xe[b]], axis=1)], axis=0)
            for i in range(4):
                s = jnp.dot(lhs, xr[tb + 4 * g + i], preferred_element_type=jnp.float32)
                e = jnp.minimum(s, 0.0) * c2 + ls
                dst[4 * g + i] = jnp.exp2(e).astype(jnp.bfloat16)
                yield

    def kv(d, src):
        a0, b0, a1, b1, tb = d
        for g, (a, b) in enumerate(((a0, b0), (a1, b1))):
            lhs = jnp.concatenate([vb[a], vb[b]], axis=1)
            for i in range(4):
                y[tb + 4 * g + i] += jnp.dot(lhs, src[4 * g + i], preferred_element_type=jnp.float32)
                yield

    def run(cur, prev, dst, src):
        gs, ks = gram(cur, dst), kv(prev, src)
        for i in range(8):
            next(gs)
            next(ks)

    def arrive(q):
        for s in (LFT + q, RGT + q):
            remote(xb.at[s], xb.at[s], sx.at[0], rx.at[s], sib).wait_recv()
            remote(vb.at[s], vb.at[s], sv.at[0], rv.at[s], sib).wait_recv()
        for c in fwd(q):
            c.start()

    def arrive2(q):
        for s in (LFT2 + q, RGT2 + q):
            remote(xb.at[s], xb.at[s], sx.at[0], rx.at[s], sib).wait_recv()
            remote(vb.at[s], vb.at[s], sv.at[0], rv.at[s], sib).wait_recv()

    def step(t, dst, src):
        d = describe(t)
        p = describe(jnp.maximum(t - 1, 0))

        @pl.when(t == 4)
        def _():
            for c in to_sib():
                c.wait_recv()

        mid = (t >= 8) & (t < 16)
        late = jnp.maximum(t - 18, 0)
        is_late = (t >= 18) & (t <= 28)
        first = (mid & (lax.rem(t, 2) == 0)) | (is_late & (lax.rem(late, 3) == 0))
        secnd = (mid & (lax.rem(t, 2) == 1)) | (is_late & (lax.rem(late, 3) == 1))
        q = jnp.where(mid, (t - 8) // 2, 4 + late // 3)
        q = jnp.minimum(jnp.maximum(q, 0), 7)

        @pl.when(first)
        def _():
            arrive(q)

        @pl.when(secnd)
        def _():
            arrive2(q)

        pa = jnp.where(t < 8, 2 * t, jnp.where(first, LFT + q, jnp.where(secnd, LFT2 + q, 0)))
        pb = jnp.where(t < 8, 2 * t + 1, jnp.where(first, RGT + q, jnp.where(secnd, RGT2 + q, 1)))

        @pl.when(t == 16)
        def _():
            lax.fori_loop(0, 4, lambda i, _: (target(RGT + i, 8 + i), 0)[1], 0)
            lax.fori_loop(0, 4, lambda i, _: (target(LFT + i, 12 + i), 0)[1], 0)

        xe[pa] = ext_rows(xb[pa], 0)
        xe[pb] = ext_rows(xb[pb], 0)
        run(d, p, dst, src)

        @pl.when(t == 29)
        def _():
            for i in range(8):
                part[i] = y[8 + i]
            for c in partial_copies():
                c.start()

    def body(u, _):
        step(2 * u, ka, kb)
        step(2 * u + 1, kb, ka)
        return 0

    lax.fori_loop(0, N_STEPS // 2, body, 0)
    for _ in kv(describe(jnp.int32(N_STEPS - 1)), kb):
        pass

    for c in partial_copies():
        c.wait()
    for i in range(8):
        out_ref[:, i * CH:(i + 1) * CH] = y[i] + pin[i]

    for q in range(8):
        for c in to_left(q, (q + 4) % 8) + to_right(q, q) + fwd(q):
            c.wait_send()
    for c in to_sib():
        c.wait_send()


def solution(mesh):
    n = mesh.shape["group"]
    row_spec = P(("tasks", "group"), None)

    def local_fn(x_loc, v_loc, lengthscale, outscale):
        rows, feat = x_loc.shape
        rhs = v_loc.shape[1]
        nc = rows // CH
        x3 = x_loc.reshape(nc, CH, feat)
        vt = v_loc.reshape(nc, CH, rhs).transpose(0, 2, 1)
        two_ell_sq = 2.0 * jnp.square(lengthscale[0])
        sc = jnp.stack([two_ell_sq, outscale[0], 2.0 * LOG2E / two_ell_sq, jnp.log2(outscale[0])])
        bf = jnp.bfloat16
        dma = pltpu.SemaphoreType.DMA
        yt = pl.pallas_call(
            functools.partial(kernel, n),
            out_shape=jax.ShapeDtypeStruct((rhs, rows), jnp.float32),
            in_specs=[pl.BlockSpec(memory_space=pl.ANY), pl.BlockSpec(memory_space=pl.ANY),
                      pl.BlockSpec(memory_space=pltpu.SMEM)],
            out_specs=pl.BlockSpec(memory_space=pltpu.VMEM),
            scratch_shapes=[
                pltpu.VMEM((6 * nc, CH, feat), bf),
                pltpu.VMEM((6 * nc, rhs, CH), bf),
                pltpu.VMEM((6 * nc, CH, 128), bf),
                pltpu.VMEM((2 * nc, feat + 128, CH), bf),
                pltpu.VMEM((nc, 2 * CH, CH), bf),
                pltpu.VMEM((nc, 2 * CH, CH), bf),
                pltpu.VMEM((2 * nc, rhs, CH), jnp.float32),
                pltpu.VMEM((nc, rhs, CH), jnp.float32),
                pltpu.VMEM((nc, rhs, CH), jnp.float32),
                dma((2,)), dma((40,)), dma((40,)), dma((6 * nc,)), dma((6 * nc,)), dma((2,)), dma((2,)),
            ],
            compiler_params=pltpu.CompilerParams(
                collective_id=0, has_side_effects=True, vmem_limit_bytes=56 * 2**20),
        )(x3, vt, sc)
        return yt.T

    return jax.shard_map(local_fn, mesh=mesh, in_specs=(row_spec, row_spec, P(None), P(None)),
                         out_specs=row_spec, check_vma=False)
```

```python
import functools

import jax
import jax.numpy as jnp
from jax import lax
from jax.experimental import pallas as pl
from jax.experimental.pallas import tpu as pltpu
from jax.sharding import PartitionSpec as P

CH = 256
LOG2E = 1.4426950408889634
OWN, SIB, LFT, RGT, LFT2, RGT2 = 0, 8, 16, 24, 32, 40
MAIN_BLOCKS = 14
LATE_STEPS = (("F", 0), ("F", 1), ("F", 2), ("F", 3), ("F", 4), ("A", 4),
              ("F", 5), ("B", 4), ("A", 5), ("B", 5), ("F", 6), ("A", 6))


def ext_values(x):
    xf = x.astype(jnp.float32)
    h = -0.5 * jnp.sum(xf * xf, axis=1, keepdims=True)
    hi = h.astype(jnp.bfloat16).astype(jnp.float32)
    r = jnp.where(h == hi, 0.0, h - hi)
    mid = r.astype(jnp.bfloat16).astype(jnp.float32)
    return hi, mid, r - mid


def ext_rows(x, *firsts):
    hi, mid, lo = ext_values(x)
    lane = lax.broadcasted_iota(jnp.int32, (x.shape[0], 128), 1)
    ones = jnp.where(lane < 6, 1.0, 0.0)
    out = []
    for first in firsts:
        e = jnp.where(lane == first, hi, ones)
        e = jnp.where(lane == first + 1, mid, e)
        e = jnp.where(lane == first + 2, lo, e)
        out.append(e.astype(jnp.bfloat16))
    return out


PREP = [(0, 1, 0, 1), (0, 1, 0, 1), (8, 9, 10, 11), (12, 13, 14, 15)]
PREP += [(LFT + q, RGT + q, LFT2 + q, RGT2 + q) for q in range(4)]
PREP += [(0, 1, 0, 1), (0, 1, LFT + 4, RGT + 4), (LFT2 + 4, RGT2 + 4, LFT + 5, RGT + 5),
         (LFT2 + 5, RGT2 + 5, 0, 1), (0, 1, LFT + 6, RGT + 6), (LFT2 + 6, RGT2 + 6, 0, 1)]


def pick(t, first, values):
    out = jnp.int32(values[0])
    for k, v in enumerate(values[1:], 1):
        if v != values[k - 1]:
            out = jnp.where(t >= first + k, jnp.int32(v), out)
    return out


def far_step(q):
    return LFT + q, LFT2 + q, RGT + q, RGT2 + q, 8


def own_step(a, b):
    return a, b, a, b, 0


def describe(t):
    w = jnp.where
    kind = pick(t, 16, ["ABF".index(k) for k, _ in LATE_STEPS])
    late_q = pick(t, 16, [q for _, q in LATE_STEPS])
    is_far = (t >= 16) & (kind == 2)
    q = w(t >= 16, late_q, jnp.maximum(t - 8, 0) // 2)
    second = w(t >= 16, kind, lax.rem(t, 2)) == 1
    a = w(t < 8, 2 * t, w(second, LFT2, LFT) + q)
    b = w(t < 8, 2 * t + 1, w(second, RGT2, RGT) + q)
    return tuple(w(is_far, f, o) for f, o in zip(far_step(q), own_step(a, b)))


def kernel(n, x_hbm, v_hbm, ell_ref, s_ref, out_ref,
           xb, vb, xe, xr, ka, kb, y, pin, cst,
           loc_sem, sx, sv, rx, rv, ps, pr):
    me = lax.axis_index("group")
    core = lax.rem(me, 2)
    sib = me + 1 - 2 * core
    left = lax.rem(me + n - 2, n)
    right = lax.rem(me + 2, n)

    def remote(src, dst, ssem, rsem, dev):
        return pltpu.make_async_remote_copy(
            src_ref=src, dst_ref=dst, send_sem=ssem, recv_sem=rsem,
            device_id={"group": dev}, device_id_type=pl.DeviceIdType.MESH)

    own_x = pltpu.make_async_copy(x_hbm, xb.at[pl.ds(OWN, 8)], loc_sem.at[0])
    own_v = [pltpu.make_async_copy(v_hbm.at[:, pl.ds(i * CH, CH)], vb.at[OWN + i], loc_sem.at[1 + i])
             for i in range(8)]
    own_x.start()
    for c in own_v:
        c.start()
    barrier = pltpu.get_barrier_semaphore()
    for dev in (sib, left, right):
        pl.semaphore_signal(barrier, inc=1, device_id={"group": dev},
                            device_id_type=pl.DeviceIdType.MESH)
    y[...] = jnp.zeros_like(y)
    kb[...] = jnp.zeros_like(kb)
    ell = jnp.full((8, CH), ell_ref[0], jnp.float32)
    cst[0:8, :] = (2.0 * LOG2E) / (2.0 * ell * ell)
    cst[8:16, :] = jnp.log2(jnp.full((8, CH), s_ref[0], jnp.float32))
    own_x.wait()

    def target_ext(slot, tile):
        e, = ext_rows(xb[slot], 3)
        xr[tile] = jnp.concatenate([xb[slot], e], axis=1).T
        return 0

    def own_ext(i, _):
        xe[i], e = ext_rows(xb[i], 0, 3)
        xr[i] = jnp.concatenate([xb[i], e], axis=1).T
        return 0

    lax.fori_loop(0, 8, own_ext, 0)
    for c in own_v:
        c.wait()
    pl.semaphore_wait(barrier, 3)

    def to_left(q, o):
        return (remote(xb.at[OWN + o], xb.at[LFT + q], sx.at[q], rx.at[LFT + q], left),
                remote(vb.at[OWN + o], vb.at[LFT + q], sv.at[q], rv.at[LFT + q], left))

    def to_right(q, o):
        return (remote(xb.at[OWN + o], xb.at[RGT + q], sx.at[8 + q], rx.at[RGT + q], right),
                remote(vb.at[OWN + o], vb.at[RGT + q], sv.at[8 + q], rv.at[RGT + q], right))

    def to_sib():
        return (remote(xb.at[pl.ds(OWN, 8)], xb.at[pl.ds(SIB, 8)], sx.at[16], rx.at[SIB], sib),
                remote(vb.at[pl.ds(OWN, 8)], vb.at[pl.ds(SIB, 8)], sv.at[16], rv.at[SIB], sib))

    def fwd(q):
        return (remote(xb.at[LFT + q], xb.at[LFT2 + q], sx.at[17 + q], rx.at[LFT2 + q], sib),
                remote(vb.at[LFT + q], vb.at[LFT2 + q], sv.at[17 + q], rv.at[LFT2 + q], sib),
                remote(xb.at[RGT + q], xb.at[RGT2 + q], sx.at[25 + q], rx.at[RGT2 + q], sib),
                remote(vb.at[RGT + q], vb.at[RGT2 + q], sv.at[25 + q], rv.at[RGT2 + q], sib))

    def partial_copies(i):
        return (remote(y.at[8 + i], pin.at[i], ps.at[i], pr.at[i], left),
                remote(y.at[12 + i], pin.at[4 + i], ps.at[4 + i], pr.at[4 + i], right))

    for q in range(8):
        for c in to_left(q, (q + 4) % 8) + to_right(q, q):
            c.start()
        if q == 0:
            for c in to_sib():
                c.start()

    def arrive(q):
        for s in (LFT + q, RGT + q):
            remote(xb.at[s], xb.at[s], sx.at[0], rx.at[s], sib).wait_recv()
            remote(vb.at[s], vb.at[s], sv.at[0], rv.at[s], sib).wait_recv()
        for c in fwd(q):
            c.start()

    def arrive2(q):
        for s in (LFT2 + q, RGT2 + q):
            remote(xb.at[s], xb.at[s], sx.at[0], rx.at[s], sib).wait_recv()
            remote(vb.at[s], vb.at[s], sv.at[0], rv.at[s], sib).wait_recv()

    def prep(slots):
        for s in slots:
            xe[s], = ext_rows(xb[s], 0)

    def dot(a, b):
        return jnp.dot(a, b, preferred_element_type=jnp.float32)

    def ext_lhs(slots):
        return jnp.concatenate([jnp.concatenate([xb[s], xe[s]], axis=1) for s in slots], axis=0)

    def k_tile(lhs, tile):
        e = jnp.minimum(dot(lhs, xr[tile]), 0.0) * cst[0:1, :] + cst[8:9, :]
        return jnp.exp2(e).astype(jnp.bfloat16)

    def kv(prev, src, i):
        g = i // 4
        lhs = jnp.concatenate([vb[prev[2 * g]], vb[prev[2 * g + 1]]], axis=1)
        y[prev[4] + i] += dot(lhs, src[i])

    def step(cur, prev, dst, src, halves=2, lag=2):
        for i in range(8):
            g = i // 4
            dst[i, 0:halves * CH, :] = k_tile(ext_lhs(cur[2 * g:2 * g + halves]), cur[4] + i)
            if src is not None and i >= lag:
                kv(prev, src, i - lag)
        if src is not None:
            for i in range(8 - lag, 8):
                kv(prev, src, i)

    def kv_only(prev, src):
        for i in range(8):
            kv(prev, src, i)

    def far_tail(tiles):
        for i in tiles:
            for m, (near, far) in enumerate(((LFT + 7, LFT2 + 7), (RGT + 7, RGT2 + 7))):
                tile = 4 * m + i
                k = k_tile(ext_lhs((far,)), 8 + tile)
                y[8 + tile] += dot(vb[near], ka[tile, 0:CH, :]) + dot(vb[far], k)

    def block(b, _):
        @pl.when(b == 2)
        def _():
            for c in to_sib():
                c.wait_recv()

        qa = pick(b, 3, (0, 1, 0, 2, 3, 3, 4, 5, 5, 6, 6))
        @pl.when((b == 3) | (b == 4) | (b == 6) | (b == 7) | (b == 9) | (b == 10) | (b == 12))
        def _():
            arrive(qa)

        qb = pick(b, 4, (0, 1, 2, 3, 3, 3, 4, 5, 5, 6))
        @pl.when(((b >= 4) & (b <= 7)) | (b == 10) | (b == 11) | (b == 13))
        def _():
            arrive2(qb)

        @pl.when(b == 8)
        def _():
            lax.fori_loop(0, 4, lambda i, _: target_ext(RGT + i, 8 + i), 0)
            lax.fori_loop(0, 4, lambda i, _: target_ext(LFT + i, 12 + i), 0)

        t = 2 * b
        d0, d1, p = describe(t), describe(t + 1), describe(jnp.maximum(t - 1, 0))
        sl = [pick(b, 0, [row[k] for row in PREP]) for k in range(4)]
        prep(sl[0:2])
        step(d0, p, ka, kb)
        prep(sl[2:4])
        step(d1, d0, kb, ka)
        return 0

    lax.fori_loop(0, MAIN_BLOCKS, block, 0)
    last = describe(jnp.int32(2 * MAIN_BLOCKS - 1))
    i32 = jnp.int32
    b6, f7 = own_step(i32(LFT2 + 6), i32(RGT2 + 6)), far_step(i32(7))
    a7, b7 = own_step(i32(LFT + 7), i32(RGT + 7)), own_step(i32(LFT2 + 7), i32(RGT2 + 7))
    arrive(7)
    prep((LFT + 7, RGT + 7))
    step(f7, last, ka, kb, halves=1)
    arrive2(7)
    prep((LFT2 + 7, RGT2 + 7))
    for j in range(2):
        far_tail((2 * j, 2 * j + 1))
        for i in (2 * j, 2 * j + 1):
            for c in partial_copies(i):
                c.start()
    step(b6, None, kb, None)
    step(a7, b6, ka, kb)
    step(b7, a7, kb, ka)
    kv_only(b7, kb)

    for q in range(8):
        for c in to_left(q, (q + 4) % 8) + to_right(q, q) + fwd(q):
            c.wait_send()
    for c in to_sib():
        c.wait_send()
    for i in range(4):
        for c in partial_copies(i):
            c.wait()
        for k in (i, 4 + i):
            out_ref[:, k * CH:(k + 1) * CH] = y[k] + pin[k]


def solution(mesh):
    n = mesh.shape["group"]
    row_spec = P(("tasks", "group"), None)

    def local_fn(x_loc, v_loc, lengthscale, outscale):
        rows, feat = x_loc.shape
        rhs = v_loc.shape[1]
        nc = rows // CH
        bf = jnp.bfloat16
        dma = pltpu.SemaphoreType.DMA
        out = pl.pallas_call(
            functools.partial(kernel, n),
            out_shape=pltpu.VMEM((rhs, rows), jnp.float32),
            in_specs=[pl.BlockSpec(memory_space=pl.ANY), pl.BlockSpec(memory_space=pl.ANY),
                      pl.BlockSpec(memory_space=pltpu.SMEM), pl.BlockSpec(memory_space=pltpu.SMEM)],
            out_specs=pl.BlockSpec(memory_space=pltpu.VMEM),
            scratch_shapes=[
                pltpu.VMEM((6 * nc, CH, feat), bf),
                pltpu.VMEM((6 * nc, rhs, CH), bf),
                pltpu.VMEM((6 * nc, CH, 128), bf),
                pltpu.VMEM((2 * nc, feat + 128, CH), bf),
                pltpu.VMEM((nc, 2 * CH, CH), bf),
                pltpu.VMEM((nc, 2 * CH, CH), bf),
                pltpu.VMEM((2 * nc, rhs, CH), jnp.float32),
                pltpu.VMEM((nc, rhs, CH), jnp.float32),
                pltpu.VMEM((16, CH), jnp.float32),
                dma((9,)), dma((40,)), dma((40,)), dma((6 * nc,)), dma((6 * nc,)), dma((8,)), dma((8,)),
            ],
            compiler_params=pltpu.CompilerParams(
                collective_id=0, has_side_effects=True, vmem_limit_bytes=56 * 2**20),
        )(x_loc.reshape(nc, CH, feat), v_loc.T, lengthscale, outscale)
        return out.T

    return jax.shard_map(local_fn, mesh=mesh, in_specs=(row_spec, row_spec, P(None), P(None)),
                         out_specs=row_spec, check_vma=False)
```

```python
import functools

import jax
import jax.numpy as jnp
from jax import lax
from jax.experimental import pallas as pl
from jax.experimental.pallas import tpu as pltpu
from jax.sharding import PartitionSpec as P

CH = 256
LOG2E = 1.4426950408889634
OWN, SIB, LFT, RGT, LFT2, RGT2 = 0, 8, 16, 24, 32, 40
BLOCKS = 16
LATE_STEPS = (("F", 0), ("F", 1), ("F", 2), ("F", 3), ("F", 4), ("F", 5), ("A", 4), ("B", 4),
              ("F", 6), ("A", 5), ("F", 7), ("B", 5), ("A", 6), ("B", 6), ("A", 7), ("B", 7))
ARRIVE = {3: 0, 4: 1, 5: 2, 7: 3, 8: 4, 9: 5, 11: 6, 12: 7}
ARRIVE2 = {4: 0, 5: 1, 6: 2, 7: 3, 9: 4, 10: 5, 12: 6, 13: 7}
SEND_BLOCK = 14


def half_norms(x):
    xf = x.astype(jnp.float32)
    h = -0.5 * jnp.sum(xf * xf, axis=1, keepdims=True)
    return jnp.broadcast_to(h, (x.shape[0], 128)).T[0:1, :]


def ext_rows(h, first):
    hi = h.astype(jnp.bfloat16).astype(jnp.float32)
    r = jnp.where(h == hi, 0.0, h - hi)
    mid = r.astype(jnp.bfloat16).astype(jnp.float32)
    lo = r - mid
    row = lax.broadcasted_iota(jnp.int32, (8, h.shape[1]), 0)
    e = jnp.where(row < 6, 1.0, 0.0)
    for k, v in enumerate((hi, mid, lo)):
        e = jnp.where(row == first + k, v, e)
    return jnp.concatenate([e, jnp.zeros((120, h.shape[1]), jnp.float32)], axis=0)


PREP = [(0, 1, 2, 3), (4, 5, 6, 7), (8, 9, 10, 11), (12, 13, 14, 15)]
PREP += [(LFT + q, RGT + q, LFT2 + q, RGT2 + q) for q in range(4)]
PREP += [(0, 1, LFT + 4, RGT + 4), (LFT2 + 4, RGT2 + 4, LFT + 5, RGT + 5), (LFT2 + 5, RGT2 + 5, 0, 1),
         (LFT + 6, RGT + 6, 0, 1), (LFT2 + 6, RGT2 + 6, LFT + 7, RGT + 7), (LFT2 + 7, RGT2 + 7, 0, 1),
         (0, 1, 0, 1), (0, 1, 0, 1)]


def pick(t, first, values):
    out = jnp.int32(values[0])
    for k, v in enumerate(values[1:], 1):
        if v != values[k - 1]:
            out = jnp.where(t >= first + k, jnp.int32(v), out)
    return out


def among(b, keys):
    hit = b == keys[0]
    for k in keys[1:]:
        hit = hit | (b == k)
    return hit


def at_block(b, table):
    out, prev = [], min(table.values())
    for k in range(BLOCKS):
        prev = table.get(k, prev)
        out.append(prev)
    return pick(b, 0, out)


def far_step(q):
    return LFT + q, LFT2 + q, RGT + q, RGT2 + q, 8


def own_step(a, b):
    return a, b, a, b, 0


def describe(t):
    w = jnp.where
    kind = pick(t, 16, ["ABF".index(k) for k, _ in LATE_STEPS])
    late_q = pick(t, 16, [q for _, q in LATE_STEPS])
    is_far = (t >= 16) & (kind == 2)
    q = w(t >= 16, late_q, jnp.maximum(t - 8, 0) // 2)
    second = w(t >= 16, kind, lax.rem(t, 2)) == 1
    a = w(t < 8, 2 * t, w(second, LFT2, LFT) + q)
    b = w(t < 8, 2 * t + 1, w(second, RGT2, RGT) + q)
    return tuple(w(is_far, f, o) for f, o in zip(far_step(q), own_step(a, b)))


def kernel(n, x_hbm, v_hbm, ell_ref, s_ref, out_ref,
           xb, vb, hb, xe, xr, ka, kb, y, pin, cst,
           loc_sem, sx, sv, sh, rx, rv, rh, ps, pr):
    me = lax.axis_index("group")
    core = lax.rem(me, 2)
    sib = me + 1 - 2 * core
    left = lax.rem(me + n - 2, n)
    right = lax.rem(me + 2, n)

    def remote(src, dst, ssem, rsem, dev):
        return pltpu.make_async_remote_copy(
            src_ref=src, dst_ref=dst, send_sem=ssem, recv_sem=rsem,
            device_id={"group": dev}, device_id_type=pl.DeviceIdType.MESH)

    own_x = pltpu.make_async_copy(x_hbm, xb.at[pl.ds(OWN, 8)], loc_sem.at[0])
    own_v = [pltpu.make_async_copy(v_hbm.at[:, pl.ds(i * CH, CH)], vb.at[OWN + i], loc_sem.at[1 + i])
             for i in range(8)]
    own_x.start()
    for c in own_v:
        c.start()
    barrier = pltpu.get_barrier_semaphore()
    for dev in (sib, left, right):
        pl.semaphore_signal(barrier, inc=1, device_id={"group": dev},
                            device_id_type=pl.DeviceIdType.MESH)
    y[...] = jnp.zeros_like(y)
    kb[...] = jnp.zeros_like(kb)
    ell = jnp.full((8, CH), ell_ref[0], jnp.float32)
    cst[0:8, :] = (2.0 * LOG2E) / (2.0 * ell * ell)
    cst[8:16, :] = jnp.log2(jnp.full((8, CH), s_ref[0], jnp.float32))
    own_x.wait()

    def target(slot, tile):
        xr[tile, 0:384, :] = xb[slot].T
        xr[tile, 384:512, :] = ext_rows(hb[slot], 3).astype(jnp.bfloat16)
        return 0

    def prep(slots):
        for s in slots:
            xe[s] = ext_rows(hb[s], 0).T.astype(jnp.bfloat16)

    def own_ext(i, _):
        hb[i] = half_norms(xb[i])
        return 0

    lax.fori_loop(0, 8, own_ext, 0)
    for c in own_v:
        c.wait()
    pl.semaphore_wait(barrier, 3)

    def rows_copy(src, dst, k, dev, count=None):
        s, d = (src, dst) if count is None else (pl.ds(src, count), pl.ds(dst, count))
        return tuple(remote(buf.at[s], buf.at[d], ss.at[k], rs.at[dst - SIB], dev)
                     for buf, ss, rs in ((hb, sh, rh), (xb, sx, rx), (vb, sv, rv)))

    def to_left(q, o):
        return rows_copy(OWN + o, LFT + q, 0, left)

    def to_right(q, o):
        return rows_copy(OWN + o, RGT + q, 1, right)

    def to_sib():
        return rows_copy(OWN, SIB, 2, sib, 8)

    def fwd(q):
        return rows_copy(LFT + q, LFT2 + q, 3, sib) + rows_copy(RGT + q, RGT2 + q, 4, sib)

    def all_sent():
        for k, (s, d, dev) in enumerate(((OWN, LFT, left), (OWN, RGT, right), (OWN, SIB, sib),
                                         (LFT, LFT2, sib), (RGT, RGT2, sib))):
            for c in rows_copy(s, d, k, dev, 8):
                c.wait_send()

    def partial_copies():
        return (remote(y.at[pl.ds(8, 4)], pin.at[pl.ds(0, 4)], ps.at[0], pr.at[0], left),
                remote(y.at[pl.ds(12, 4)], pin.at[pl.ds(4, 4)], ps.at[1], pr.at[1], right))

    for q in range(8):
        for c in to_left(q, (q + 4) % 8) + to_right(q, q):
            c.start()
        if q == 0:
            for c in to_sib():
                c.start()

    def received(slot):
        for c in rows_copy(slot, slot, 0, sib):
            c.wait_recv()

    def arrive(q):
        received(LFT + q)
        received(RGT + q)
        for c in fwd(q):
            c.start()

    def arrive2(q):
        received(LFT2 + q)
        received(RGT2 + q)

    lax.fori_loop(0, 8, lambda i, _: target(OWN + i, i), 0)

    def dot(a, b):
        return jnp.dot(a, b, preferred_element_type=jnp.float32)

    def ext_lhs(slots):
        return jnp.concatenate([jnp.concatenate([xb[s], xe[s]], axis=1) for s in slots], axis=0)

    def k_tile(lhs, tile):
        e = jnp.minimum(dot(lhs, xr[tile]), 0.0) * cst[0:1, :] + cst[8:9, :]
        return jnp.exp2(e).astype(jnp.bfloat16)

    def kv(prev, src, i):
        g = i // 4
        lhs = jnp.concatenate([vb[prev[2 * g]], vb[prev[2 * g + 1]]], axis=1)
        y[prev[4] + i] += dot(lhs, src[i])

    def step(cur, prev, dst, src, halves=2, lag=2):
        for i in range(8):
            g = i // 4
            dst[i, 0:halves * CH, :] = k_tile(ext_lhs(cur[2 * g:2 * g + halves]), cur[4] + i)
            if src is not None and i >= lag:
                kv(prev, src, i - lag)
        if src is not None:
            for i in range(8 - lag, 8):
                kv(prev, src, i)

    def block(b, _):
        @pl.when(b == 2)
        def _():
            for c in to_sib():
                c.wait_recv()

        @pl.when(among(b, tuple(ARRIVE)))
        def _():
            arrive(at_block(b, ARRIVE))

        @pl.when(among(b, tuple(ARRIVE2)))
        def _():
            arrive2(at_block(b, ARRIVE2))

        @pl.when(b == SEND_BLOCK)
        def _():
            for c in partial_copies():
                c.start()

        @pl.when(b == 8)
        def _():
            lax.fori_loop(0, 4, lambda i, _: target(RGT + i, 8 + i), 0)
            lax.fori_loop(0, 4, lambda i, _: target(LFT + i, 12 + i), 0)

        t = 2 * b
        d0, d1, p = describe(t), describe(t + 1), describe(jnp.maximum(t - 1, 0))
        sl = [pick(b, 0, [row[k] for row in PREP]) for k in range(4)]
        prep(sl[0:2])
        step(d0, p, ka, kb)
        prep(sl[2:4])
        step(d1, d0, kb, ka)
        return 0

    lax.fori_loop(0, BLOCKS, block, 0)
    i32 = jnp.int32
    last = own_step(i32(LFT2 + 7), i32(RGT2 + 7))
    for i in range(8):
        kv(last, kb, i)
    all_sent()
    for c in partial_copies():
        c.wait()
    for i in range(8):
        out_ref[:, i * CH:(i + 1) * CH] = y[i] + pin[i]


def solution(mesh):
    n = mesh.shape["group"]
    row_spec = P(("tasks", "group"), None)

    def local_fn(x_loc, v_loc, lengthscale, outscale):
        rows, feat = x_loc.shape
        rhs = v_loc.shape[1]
        nc = rows // CH
        bf = jnp.bfloat16
        dma = pltpu.SemaphoreType.DMA
        out = pl.pallas_call(
            functools.partial(kernel, n),
            out_shape=pltpu.VMEM((rhs, rows), jnp.float32),
            in_specs=[pl.BlockSpec(memory_space=pl.ANY), pl.BlockSpec(memory_space=pl.ANY),
                      pl.BlockSpec(memory_space=pltpu.SMEM), pl.BlockSpec(memory_space=pltpu.SMEM)],
            out_specs=pl.BlockSpec(memory_space=pltpu.VMEM),
            scratch_shapes=[
                pltpu.VMEM((6 * nc, CH, feat), bf),
                pltpu.VMEM((6 * nc, rhs, CH), bf),
                pltpu.VMEM((6 * nc, 1, CH), jnp.float32),
                pltpu.VMEM((6 * nc, CH, 128), bf),
                pltpu.VMEM((2 * nc, feat + 128, CH), bf),
                pltpu.VMEM((nc, 2 * CH, CH), bf),
                pltpu.VMEM((nc, 2 * CH, CH), bf),
                pltpu.VMEM((2 * nc, rhs, CH), jnp.float32),
                pltpu.VMEM((nc, rhs, CH), jnp.float32),
                pltpu.VMEM((16, CH), jnp.float32),
                dma((9,)), dma((5,)), dma((5,)), dma((5,)), dma((5 * nc,)), dma((5 * nc,)), dma((5 * nc,)),
                dma((2,)), dma((2,)),
            ],
            compiler_params=pltpu.CompilerParams(
                collective_id=0, has_side_effects=True, vmem_limit_bytes=56 * 2**20),
        )(x_loc.reshape(nc, CH, feat), v_loc.T, lengthscale, outscale)
        return out.T

    return jax.shard_map(local_fn, mesh=mesh, in_specs=(row_spec, row_spec, P(None), P(None)),
                         out_specs=row_spec, check_vma=False)
```

```python
import functools

import jax
import jax.numpy as jnp
from jax import lax
from jax.experimental import pallas as pl
from jax.experimental.pallas import tpu as pltpu
from jax.sharding import PartitionSpec as P

CH = 256
LOG2E = 1.4426950408889634
OWN, SIB, LFT, RGT, LFT2, RGT2 = 0, 8, 16, 24, 32, 40
BLOCKS = 16
LATE_STEPS = (("F", 0), ("F", 1), ("F", 2), ("F", 3), ("F", 4), ("F", 5), ("A", 4), ("B", 4),
              ("F", 6), ("A", 5), ("F", 7), ("B", 5), ("A", 6), ("B", 6), ("A", 7), ("B", 7))
GROUPS = ((0, 2), (2, 2), (4, 2), (6, 1), (7, 1))
ARRIVE = {2: {4: 0, 6: 2, 9: 4}, 1: {11: 6, 12: 7}}
ARRIVE2 = {2: {5: 0, 7: 2, 10: 4}, 1: {12: 6, 13: 7}}
SEND_BLOCK = 14


def half_norms(x):
    xf = x.astype(jnp.float32)
    h = -0.5 * jnp.sum(xf * xf, axis=1, keepdims=True)
    return jnp.broadcast_to(h, (x.shape[0], 128)).T[0:1, :]


def ext_rows(h, first):
    hi = h.astype(jnp.bfloat16).astype(jnp.float32)
    r = jnp.where(h == hi, 0.0, h - hi)
    mid = r.astype(jnp.bfloat16).astype(jnp.float32)
    lo = r - mid
    row = lax.broadcasted_iota(jnp.int32, (8, h.shape[1]), 0)
    e = jnp.where(row < 6, 1.0, 0.0)
    for k, v in enumerate((hi, mid, lo)):
        e = jnp.where(row == first + k, v, e)
    return jnp.concatenate([e, jnp.zeros((120, h.shape[1]), jnp.float32)], axis=0)


PREP = [(0, 1, 2, 3), (4, 5, 6, 7), (8, 9, 10, 11), (12, 13, 14, 15)]
PREP += [(a + q, b + q, a + q + 1, b + q + 1) for q in (0, 2) for a, b in ((LFT, RGT), (LFT2, RGT2))]
PREP += [(0, 1, 0, 1), (LFT + 4, RGT + 4, LFT + 5, RGT + 5), (LFT2 + 4, RGT2 + 4, LFT2 + 5, RGT2 + 5),
         (LFT + 6, RGT + 6, 0, 1), (LFT2 + 6, RGT2 + 6, LFT + 7, RGT + 7), (LFT2 + 7, RGT2 + 7, 0, 1),
         (0, 1, 0, 1), (0, 1, 0, 1)]


def pick(t, first, values):
    out = jnp.int32(values[0])
    for k, v in enumerate(values[1:], 1):
        if v != values[k - 1]:
            out = jnp.where(t >= first + k, jnp.int32(v), out)
    return out


def among(b, keys):
    hit = b == keys[0]
    for k in keys[1:]:
        hit = hit | (b == k)
    return hit


def at_block(b, table):
    out, prev = [], min(table.values())
    for k in range(BLOCKS):
        prev = table.get(k, prev)
        out.append(prev)
    return pick(b, 0, out)


def far_step(q):
    return LFT + q, LFT2 + q, RGT + q, RGT2 + q, 8


def own_step(a, b):
    return a, b, a, b, 0


def describe(t):
    w = jnp.where
    kind = pick(t, 16, ["ABF".index(k) for k, _ in LATE_STEPS])
    late_q = pick(t, 16, [q for _, q in LATE_STEPS])
    is_far = (t >= 16) & (kind == 2)
    u = jnp.maximum(t - 8, 0)
    q = w(t >= 16, late_q, 2 * (u // 4) + lax.rem(u, 2))
    second = w(t >= 16, kind, lax.rem(u // 2, 2)) == 1
    a = w(t < 8, 2 * t, w(second, LFT2, LFT) + q)
    b = w(t < 8, 2 * t + 1, w(second, RGT2, RGT) + q)
    return tuple(w(is_far, f, o) for f, o in zip(far_step(q), own_step(a, b)))


def kernel(n, x_hbm, v_hbm, ell_ref, s_ref, out_ref,
           xb, vb, hb, xe, xr, ka, kb, y, pin, cst,
           loc_sem, sx, sv, sh, rx, rv, rh, ps, pr):
    me = lax.axis_index("group")
    core = lax.rem(me, 2)
    sib = me + 1 - 2 * core
    left = lax.rem(me + n - 2, n)
    right = lax.rem(me + 2, n)

    def remote(src, dst, ssem, rsem, dev):
        return pltpu.make_async_remote_copy(
            src_ref=src, dst_ref=dst, send_sem=ssem, recv_sem=rsem,
            device_id={"group": dev}, device_id_type=pl.DeviceIdType.MESH)

    own_x = pltpu.make_async_copy(x_hbm, xb.at[pl.ds(OWN, 8)], loc_sem.at[0])
    own_v = [pltpu.make_async_copy(v_hbm.at[:, pl.ds(i * CH, CH)], vb.at[OWN + i], loc_sem.at[1 + i])
             for i in range(8)]
    own_x.start()
    for c in own_v:
        c.start()
    barrier = pltpu.get_barrier_semaphore()
    for dev in (sib, left, right):
        pl.semaphore_signal(barrier, inc=1, device_id={"group": dev},
                            device_id_type=pl.DeviceIdType.MESH)
    y[...] = jnp.zeros_like(y)
    kb[...] = jnp.zeros_like(kb)
    ell = jnp.full((8, CH), ell_ref[0], jnp.float32)
    cst[0:8, :] = (2.0 * LOG2E) / (2.0 * ell * ell)
    cst[8:16, :] = jnp.log2(jnp.full((8, CH), s_ref[0], jnp.float32))
    own_x.wait()

    def target(slot, tile):
        xr[tile, 0:384, :] = xb[slot].T
        xr[tile, 384:512, :] = ext_rows(hb[slot], 3).astype(jnp.bfloat16)
        return 0

    def prep(slots):
        for s in slots:
            xe[s] = ext_rows(hb[s], 0).T.astype(jnp.bfloat16)

    def own_ext(i, _):
        hb[i] = half_norms(xb[i])
        return 0

    lax.fori_loop(0, 8, own_ext, 0)
    for c in own_v:
        c.wait()
    pl.semaphore_wait(barrier, 3)

    def rows_copy(src, dst, k, dev, count):
        return tuple(remote(buf.at[pl.ds(src, count)], buf.at[pl.ds(dst, count)], ss.at[k], rs.at[dst - SIB], dev)
                     for buf, ss, rs in ((hb, sh, rh), (xb, sx, rx), (vb, sv, rv)))

    def to_left(q, count):
        return rows_copy(OWN + (q + 4) % 8, LFT + q, 0, left, count)

    def to_right(q, count):
        return rows_copy(OWN + q, RGT + q, 1, right, count)

    def to_sib():
        return rows_copy(OWN, SIB, 2, sib, 8)

    def fwd(q, count):
        return rows_copy(LFT + q, LFT2 + q, 3, sib, count) + rows_copy(RGT + q, RGT2 + q, 4, sib, count)

    def all_sent():
        for k, (s, d, dev) in enumerate(((OWN, LFT, left), (OWN, RGT, right), (OWN, SIB, sib),
                                         (LFT, LFT2, sib), (RGT, RGT2, sib))):
            for c in rows_copy(s, d, k, dev, 8):
                c.wait_send()

    def partial_copies():
        return (remote(y.at[pl.ds(8, 4)], pin.at[pl.ds(0, 4)], ps.at[0], pr.at[0], left),
                remote(y.at[pl.ds(12, 4)], pin.at[pl.ds(4, 4)], ps.at[1], pr.at[1], right))

    for q, count in GROUPS:
        for c in to_left(q, count) + to_right(q, count):
            c.start()
        if q == 0:
            for c in to_sib():
                c.start()

    def received(slot, count):
        for c in rows_copy(slot, slot, 0, sib, count):
            c.wait_recv()

    def arrive(q, count):
        received(LFT + q, count)
        received(RGT + q, count)
        for c in fwd(q, count):
            c.start()

    def arrive2(q, count):
        received(LFT2 + q, count)
        received(RGT2 + q, count)

    lax.fori_loop(0, 8, lambda i, _: target(OWN + i, i), 0)

    def dot(a, b):
        return jnp.dot(a, b, preferred_element_type=jnp.float32)

    def ext_lhs(slots):
        return jnp.concatenate([jnp.concatenate([xb[s], xe[s]], axis=1) for s in slots], axis=0)

    def k_tile(lhs, tile):
        e = jnp.minimum(dot(lhs, xr[tile]), 0.0) * cst[0:1, 0:1] + cst[8:9, 0:1]
        return jnp.exp2(e).astype(jnp.bfloat16)

    def kv(prev, src, i):
        g = i // 4
        lhs = jnp.concatenate([vb[prev[2 * g]], vb[prev[2 * g + 1]]], axis=1)
        y[prev[4] + i] += dot(lhs, src[i])

    def step(cur, prev, dst, src, halves=2, lag=2):
        for i in range(8):
            g = i // 4
            dst[i, 0:halves * CH, :] = k_tile(ext_lhs(cur[2 * g:2 * g + halves]), cur[4] + i)
            if src is not None and i >= lag:
                kv(prev, src, i - lag)
        if src is not None:
            for i in range(8 - lag, 8):
                kv(prev, src, i)

    def block(b, _):
        @pl.when(b == 2)
        def _():
            for c in to_sib():
                c.wait_recv()

        for table, event in ((ARRIVE, arrive), (ARRIVE2, arrive2)):
            for count, at in table.items():
                @pl.when(among(b, tuple(at)))
                def _(event=event, at=at, count=count):
                    event(at_block(b, at), count)

        @pl.when(b == SEND_BLOCK)
        def _():
            for c in partial_copies():
                c.start()

        @pl.when(b == 8)
        def _():
            lax.fori_loop(0, 4, lambda i, _: target(RGT + i, 8 + i), 0)
            lax.fori_loop(0, 4, lambda i, _: target(LFT + i, 12 + i), 0)

        t = 2 * b
        d0, d1, p = describe(t), describe(t + 1), describe(jnp.maximum(t - 1, 0))
        sl = [pick(b, 0, [row[k] for row in PREP]) for k in range(4)]
        prep(sl[0:2])
        step(d0, p, ka, kb)
        prep(sl[2:4])
        step(d1, d0, kb, ka)
        return 0

    lax.fori_loop(0, BLOCKS, block, 0)
    i32 = jnp.int32
    last = own_step(i32(LFT2 + 7), i32(RGT2 + 7))
    for i in range(8):
        kv(last, kb, i)
    all_sent()
    for c in partial_copies():
        c.wait()
    for i in range(8):
        out_ref[:, i * CH:(i + 1) * CH] = y[i] + pin[i]


def solution(mesh):
    n = mesh.shape["group"]
    row_spec = P(("tasks", "group"), None)

    def local_fn(x_loc, v_loc, lengthscale, outscale):
        rows, feat = x_loc.shape
        rhs = v_loc.shape[1]
        nc = rows // CH
        bf = jnp.bfloat16
        dma = pltpu.SemaphoreType.DMA
        out = pl.pallas_call(
            functools.partial(kernel, n),
            out_shape=pltpu.VMEM((rhs, rows), jnp.float32),
            in_specs=[pl.BlockSpec(memory_space=pl.ANY), pl.BlockSpec(memory_space=pl.ANY),
                      pl.BlockSpec(memory_space=pltpu.SMEM), pl.BlockSpec(memory_space=pltpu.SMEM)],
            out_specs=pl.BlockSpec(memory_space=pltpu.VMEM),
            scratch_shapes=[
                pltpu.VMEM((6 * nc, CH, feat), bf),
                pltpu.VMEM((6 * nc, rhs, CH), bf),
                pltpu.VMEM((6 * nc, 1, CH), jnp.float32),
                pltpu.VMEM((6 * nc, CH, 128), bf),
                pltpu.VMEM((2 * nc, feat + 128, CH), bf),
                pltpu.VMEM((nc, 2 * CH, CH), bf),
                pltpu.VMEM((nc, 2 * CH, CH), bf),
                pltpu.VMEM((2 * nc, rhs, CH), jnp.float32),
                pltpu.VMEM((nc, rhs, CH), jnp.float32),
                pltpu.VMEM((16, CH), jnp.float32),
                dma((9,)), dma((5,)), dma((5,)), dma((5,)), dma((5 * nc,)), dma((5 * nc,)), dma((5 * nc,)),
                dma((2,)), dma((2,)),
            ],
            compiler_params=pltpu.CompilerParams(
                collective_id=0, has_side_effects=True, vmem_limit_bytes=56 * 2**20),
        )(x_loc.reshape(nc, CH, feat), v_loc.T, lengthscale, outscale)
        return out.T

    return jax.shard_map(local_fn, mesh=mesh, in_specs=(row_spec, row_spec, P(None), P(None)),
                         out_specs=row_spec, check_vma=False)
```

```python
import functools

import jax
import jax.numpy as jnp
from jax import lax
from jax.experimental import pallas as pl
from jax.experimental.pallas import tpu as pltpu
from jax.sharding import PartitionSpec as P

CH = 256
LOG2E = 1.4426950408889634
OWN, SIB, LFT, RGT, LFT2, RGT2 = 0, 8, 16, 24, 32, 40
BLOCKS = 16
LATE_STEPS = (("F", 0), ("F", 1), ("F", 2), ("F", 3), ("F", 4), ("F", 5), ("A", 4), ("B", 4),
              ("F", 6), ("A", 5), ("F", 7), ("B", 5), ("A", 6), ("B", 6), ("A", 7), ("B", 7))
GROUPS = ((0, 2), (2, 2), (4, 2), (6, 1), (7, 1))
ARRIVE = {2: {4: 0, 6: 2, 9: 4}, 1: {11: 6, 12: 7}}
ARRIVE2 = {2: {5: 0, 7: 2, 10: 4}, 1: {12: 6, 13: 7}}
SEND_BLOCK = 14


def half_norms(x):
    xf = x.astype(jnp.float32)
    h = -0.5 * jnp.sum(xf * xf, axis=1, keepdims=True)
    return jnp.broadcast_to(h, (x.shape[0], 128)).T[0:1, :]


def ext_rows(h, first):
    hi = h.astype(jnp.bfloat16).astype(jnp.float32)
    r = jnp.where(h == hi, 0.0, h - hi)
    mid = r.astype(jnp.bfloat16).astype(jnp.float32)
    lo = r - mid
    row = lax.broadcasted_iota(jnp.int32, (8, h.shape[1]), 0)
    e = jnp.where(row < 6, 1.0, 0.0)
    for k, v in enumerate((hi, mid, lo)):
        e = jnp.where(row == first + k, v, e)
    return jnp.concatenate([e, jnp.zeros((120, h.shape[1]), jnp.float32)], axis=0)


PREP = [(0, 1, 2, 3), (4, 5, 6, 7), (8, 9, 10, 11), (12, 13, 14, 15)]
PREP += [(a + q, b + q, a + q + 1, b + q + 1) for q in (0, 2) for a, b in ((LFT, RGT), (LFT2, RGT2))]
PREP += [(0, 1, 0, 1), (LFT + 4, RGT + 4, LFT + 5, RGT + 5), (LFT2 + 4, RGT2 + 4, LFT2 + 5, RGT2 + 5),
         (LFT + 6, RGT + 6, 0, 1), (LFT2 + 6, RGT2 + 6, LFT + 7, RGT + 7), (LFT2 + 7, RGT2 + 7, 0, 1),
         (0, 1, 0, 1), (0, 1, 0, 1)]


def pick(t, first, values):
    out = jnp.int32(values[0])
    for k, v in enumerate(values[1:], 1):
        if v != values[k - 1]:
            out = jnp.where(t >= first + k, jnp.int32(v), out)
    return out


def among(b, keys):
    hit = b == keys[0]
    for k in keys[1:]:
        hit = hit | (b == k)
    return hit


def at_block(b, table):
    out, prev = [], min(table.values())
    for k in range(BLOCKS):
        prev = table.get(k, prev)
        out.append(prev)
    return pick(b, 0, out)


def far_step(q):
    return LFT + q, LFT2 + q, RGT + q, RGT2 + q, 8


def own_step(a, b):
    return a, b, a, b, 0


def describe(t):
    w = jnp.where
    kind = pick(t, 16, ["ABF".index(k) for k, _ in LATE_STEPS])
    late_q = pick(t, 16, [q for _, q in LATE_STEPS])
    is_far = (t >= 16) & (kind == 2)
    u = jnp.maximum(t - 8, 0)
    q = w(t >= 16, late_q, 2 * (u // 4) + lax.rem(u, 2))
    second = w(t >= 16, kind, lax.rem(u // 2, 2)) == 1
    a = w(t < 8, 2 * t, w(second, LFT2, LFT) + q)
    b = w(t < 8, 2 * t + 1, w(second, RGT2, RGT) + q)
    return tuple(w(is_far, f, o) for f, o in zip(far_step(q), own_step(a, b)))


def kernel(n, x_hbm, v_hbm, ell_ref, s_ref, out_ref,
           xb, vb, hb, xe, xr, ka, kb, y, pin, cst,
           loc_sem, sx, sv, sh, rx, rv, rh, ps, pr):
    me = lax.axis_index("group")
    core = lax.rem(me, 2)
    sib = me + 1 - 2 * core
    left = lax.rem(me + n - 2, n)
    right = lax.rem(me + 2, n)

    def remote(src, dst, ssem, rsem, dev):
        return pltpu.make_async_remote_copy(
            src_ref=src, dst_ref=dst, send_sem=ssem, recv_sem=rsem,
            device_id={"group": dev}, device_id_type=pl.DeviceIdType.MESH)

    own_x = pltpu.make_async_copy(x_hbm, xb.at[pl.ds(OWN, 8)], loc_sem.at[0])
    own_v = [pltpu.make_async_copy(v_hbm.at[:, pl.ds(i * CH, CH)], vb.at[OWN + i], loc_sem.at[1 + i])
             for i in range(8)]
    own_x.start()
    for c in own_v:
        c.start()
    barrier = pltpu.get_barrier_semaphore()
    for dev in (sib, left, right):
        pl.semaphore_signal(barrier, inc=1, device_id={"group": dev},
                            device_id_type=pl.DeviceIdType.MESH)
    y[...] = jnp.zeros_like(y)
    kb[...] = jnp.zeros_like(kb)
    ell = jnp.full((8, CH), ell_ref[0], jnp.float32)
    cst[0:8, :] = (2.0 * LOG2E) / (2.0 * ell * ell)
    cst[8:16, :] = jnp.log2(jnp.full((8, CH), s_ref[0], jnp.float32))
    own_x.wait()

    def target(slot, tile):
        xr[tile, 0:384, :] = xb[slot].T
        xr[tile, 384:512, :] = ext_rows(hb[slot], 3).astype(jnp.bfloat16)
        return 0

    def prep(slots):
        for s in slots:
            xe[s] = ext_rows(hb[s], 0).T.astype(jnp.bfloat16)

    def own_ext(i, _):
        hb[i] = half_norms(xb[i])
        return 0

    for c in own_v:
        c.wait()
    pl.semaphore_wait(barrier, 3)

    def rows_copy(src, dst, k, dev, count):
        return tuple(remote(buf.at[pl.ds(src, count)], buf.at[pl.ds(dst, count)], ss.at[k], rs.at[dst - SIB], dev)
                     for buf, ss, rs in ((hb, sh, rh), (xb, sx, rx), (vb, sv, rv)))

    def to_left(q, count):
        return rows_copy(OWN + (q + 4) % 8, LFT + q, 0, left, count)

    def to_right(q, count):
        return rows_copy(OWN + q, RGT + q, 1, right, count)

    def to_sib():
        return rows_copy(OWN, SIB, 2, sib, 8)

    def fwd(q, count):
        return rows_copy(LFT + q, LFT2 + q, 3, sib, count) + rows_copy(RGT + q, RGT2 + q, 4, sib, count)

    def all_sent():
        for k, (s, d, dev) in enumerate(((OWN, LFT, left), (OWN, RGT, right), (OWN, SIB, sib),
                                         (LFT, LFT2, sib), (RGT, RGT2, sib))):
            for c in rows_copy(s, d, k, dev, 8):
                c.wait_send()

    def partial_copies():
        return (remote(y.at[pl.ds(8, 4)], pin.at[pl.ds(0, 4)], ps.at[0], pr.at[0], left),
                remote(y.at[pl.ds(12, 4)], pin.at[pl.ds(4, 4)], ps.at[1], pr.at[1], right))

    first, rest = GROUPS[0], GROUPS[1:]
    early = [to_left(*first), to_right(*first), to_sib()]
    for c in early[0][1:] + early[1][1:] + early[2][1:]:
        c.start()
    lax.fori_loop(0, 8, own_ext, 0)
    lax.fori_loop(0, 8, lambda i, _: target(OWN + i, i), 0)
    for copies in early:
        copies[0].start()
    for q, count in rest:
        for c in to_left(q, count) + to_right(q, count):
            c.start()

    def received(slot, count):
        for c in rows_copy(slot, slot, 0, sib, count):
            c.wait_recv()

    def arrive(q, count):
        received(LFT + q, count)
        received(RGT + q, count)
        for c in fwd(q, count):
            c.start()

    def arrive2(q, count):
        received(LFT2 + q, count)
        received(RGT2 + q, count)

    def dot(a, b):
        return jnp.dot(a, b, preferred_element_type=jnp.float32)

    def ext_lhs(slots):
        return jnp.concatenate([jnp.concatenate([xb[s], xe[s]], axis=1) for s in slots], axis=0)

    def k_tile(lhs, tile):
        e = jnp.minimum(dot(lhs, xr[tile]), 0.0) * cst[0:1, 0:1] + cst[8:9, 0:1]
        return jnp.exp2(e).astype(jnp.bfloat16)

    def kv(prev, src, i):
        g = i // 4
        lhs = jnp.concatenate([vb[prev[2 * g]], vb[prev[2 * g + 1]]], axis=1)
        y[prev[4] + i] += dot(lhs, src[i])

    def step(cur, prev, dst, src, halves=2, lag=2):
        for i in range(8):
            g = i // 4
            dst[i, 0:halves * CH, :] = k_tile(ext_lhs(cur[2 * g:2 * g + halves]), cur[4] + i)
            if src is not None and i >= lag:
                kv(prev, src, i - lag)
        if src is not None:
            for i in range(8 - lag, 8):
                kv(prev, src, i)

    def block(b, _):
        @pl.when(b == 2)
        def _():
            for c in to_sib():
                c.wait_recv()

        for table, event in ((ARRIVE, arrive), (ARRIVE2, arrive2)):
            for count, at in table.items():
                @pl.when(among(b, tuple(at)))
                def _(event=event, at=at, count=count):
                    event(at_block(b, at), count)

        @pl.when(b == SEND_BLOCK)
        def _():
            for c in partial_copies():
                c.start()

        @pl.when(b == 8)
        def _():
            lax.fori_loop(0, 4, lambda i, _: target(RGT + i, 8 + i), 0)
            lax.fori_loop(0, 4, lambda i, _: target(LFT + i, 12 + i), 0)

        t = 2 * b
        d0, d1, p = describe(t), describe(t + 1), describe(jnp.maximum(t - 1, 0))
        sl = [pick(b, 0, [row[k] for row in PREP]) for k in range(4)]
        prep(sl[0:2])
        step(d0, p, ka, kb)
        prep(sl[2:4])
        step(d1, d0, kb, ka)
        return 0

    lax.fori_loop(0, BLOCKS, block, 0)
    i32 = jnp.int32
    last = own_step(i32(LFT2 + 7), i32(RGT2 + 7))
    for i in range(8):
        kv(last, kb, i)
    all_sent()
    for c in partial_copies():
        c.wait()
    for i in range(8):
        out_ref[:, i * CH:(i + 1) * CH] = y[i] + pin[i]


def solution(mesh):
    n = mesh.shape["group"]
    row_spec = P(("tasks", "group"), None)

    def local_fn(x_loc, v_loc, lengthscale, outscale):
        rows, feat = x_loc.shape
        rhs = v_loc.shape[1]
        nc = rows // CH
        bf = jnp.bfloat16
        dma = pltpu.SemaphoreType.DMA
        out = pl.pallas_call(
            functools.partial(kernel, n),
            out_shape=pltpu.VMEM((rhs, rows), jnp.float32),
            in_specs=[pl.BlockSpec(memory_space=pl.ANY), pl.BlockSpec(memory_space=pl.ANY),
                      pl.BlockSpec(memory_space=pltpu.SMEM), pl.BlockSpec(memory_space=pltpu.SMEM)],
            out_specs=pl.BlockSpec(memory_space=pltpu.VMEM),
            scratch_shapes=[
                pltpu.VMEM((6 * nc, CH, feat), bf),
                pltpu.VMEM((6 * nc, rhs, CH), bf),
                pltpu.VMEM((6 * nc, 1, CH), jnp.float32),
                pltpu.VMEM((6 * nc, CH, 128), bf),
                pltpu.VMEM((2 * nc, feat + 128, CH), bf),
                pltpu.VMEM((nc, 2 * CH, CH), bf),
                pltpu.VMEM((nc, 2 * CH, CH), bf),
                pltpu.VMEM((2 * nc, rhs, CH), jnp.float32),
                pltpu.VMEM((nc, rhs, CH), jnp.float32),
                pltpu.VMEM((16, CH), jnp.float32),
                dma((9,)), dma((5,)), dma((5,)), dma((5,)), dma((5 * nc,)), dma((5 * nc,)), dma((5 * nc,)),
                dma((2,)), dma((2,)),
            ],
            compiler_params=pltpu.CompilerParams(
                collective_id=0, has_side_effects=True, vmem_limit_bytes=56 * 2**20),
        )(x_loc.reshape(nc, CH, feat), v_loc.T, lengthscale, outscale)
        return out.T

    return jax.shard_map(local_fn, mesh=mesh, in_specs=(row_spec, row_spec, P(None), P(None)),
                         out_specs=row_spec, check_vma=False)
```

```python
import functools

import jax
import jax.numpy as jnp
from jax import lax
from jax.experimental import pallas as pl
from jax.experimental.pallas import tpu as pltpu
from jax.sharding import PartitionSpec as P

CH = 256
LOG2E = 1.4426950408889634
OWN, SIB, LFT, RGT, LFT2, RGT2 = 0, 8, 16, 24, 32, 40
BLOCKS = 16
LATE_STEPS = (("F", 0), ("F", 1), ("F", 2), ("F", 3), ("F", 4), ("F", 5), ("A", 4), ("B", 4),
              ("F", 6), ("A", 5), ("F", 7), ("B", 5), ("A", 6), ("B", 6), ("A", 7), ("B", 7))
GROUPS = ((0, 2), (2, 2), (4, 2), (6, 1), (7, 1))
ARRIVE = {2: {4: 0, 6: 2, 9: 4}, 1: {11: 6, 12: 7}}
ARRIVE2 = {2: {5: 0, 7: 2, 10: 4}, 1: {12: 6, 13: 7}}
SEND_BLOCK = 14


def half_norms(x):
    xf = x.astype(jnp.float32)
    h = -0.5 * jnp.sum(xf * xf, axis=1, keepdims=True)
    return jnp.broadcast_to(h, (x.shape[0], 128)).T[0:1, :]


def ext_rows(h, first):
    hi = h.astype(jnp.bfloat16).astype(jnp.float32)
    r = jnp.where(h == hi, 0.0, h - hi)
    mid = r.astype(jnp.bfloat16).astype(jnp.float32)
    lo = r - mid
    row = lax.broadcasted_iota(jnp.int32, (8, h.shape[1]), 0)
    e = jnp.where(row < 6, 1.0, 0.0)
    for k, v in enumerate((hi, mid, lo)):
        e = jnp.where(row == first + k, v, e)
    return jnp.concatenate([e, jnp.zeros((120, h.shape[1]), jnp.float32)], axis=0)


PREP = [(0, 1, 2, 3), (4, 5, 6, 7), (8, 9, 10, 11), (12, 13, 14, 15)]
PREP += [(a + q, b + q, a + q + 1, b + q + 1) for q in (0, 2) for a, b in ((LFT, RGT), (LFT2, RGT2))]
PREP += [(0, 1, 0, 1), (LFT + 4, RGT + 4, LFT + 5, RGT + 5), (LFT2 + 4, RGT2 + 4, LFT2 + 5, RGT2 + 5),
         (LFT + 6, RGT + 6, 0, 1), (LFT2 + 6, RGT2 + 6, LFT + 7, RGT + 7), (LFT2 + 7, RGT2 + 7, 0, 1),
         (0, 1, 0, 1), (0, 1, 0, 1)]


def pick(t, first, values):
    out = jnp.int32(values[0])
    for k, v in enumerate(values[1:], 1):
        if v != values[k - 1]:
            out = jnp.where(t >= first + k, jnp.int32(v), out)
    return out


def among(b, keys):
    hit = b == keys[0]
    for k in keys[1:]:
        hit = hit | (b == k)
    return hit


def at_block(b, table):
    out, prev = [], min(table.values())
    for k in range(BLOCKS):
        prev = table.get(k, prev)
        out.append(prev)
    return pick(b, 0, out)


def far_step(q):
    return LFT + q, LFT2 + q, RGT + q, RGT2 + q, 8


def own_step(a, b):
    return a, b, a, b, 0


def describe(t):
    w = jnp.where
    kind = pick(t, 16, ["ABF".index(k) for k, _ in LATE_STEPS])
    late_q = pick(t, 16, [q for _, q in LATE_STEPS])
    is_far = (t >= 16) & (kind == 2)
    u = jnp.maximum(t - 8, 0)
    q = w(t >= 16, late_q, 2 * (u // 4) + lax.rem(u, 2))
    second = w(t >= 16, kind, lax.rem(u // 2, 2)) == 1
    a = w(t < 8, 2 * t, w(second, LFT2, LFT) + q)
    b = w(t < 8, 2 * t + 1, w(second, RGT2, RGT) + q)
    return tuple(w(is_far, f, o) for f, o in zip(far_step(q), own_step(a, b)))


def kernel(n, x_hbm, v_hbm, ell_ref, s_ref, out_ref,
           xb, vb, hb, xe, xr, ka, kb, y, pin, cst,
           loc_sem, sx, sv, sh, rx, rv, rh, ps, pr):
    me = lax.axis_index("group")
    core = lax.rem(me, 2)
    sib = me + 1 - 2 * core
    left = lax.rem(me + n - 2, n)
    right = lax.rem(me + 2, n)

    def remote(src, dst, ssem, rsem, dev):
        return pltpu.make_async_remote_copy(
            src_ref=src, dst_ref=dst, send_sem=ssem, recv_sem=rsem,
            device_id={"group": dev}, device_id_type=pl.DeviceIdType.MESH)

    own_x = pltpu.make_async_copy(x_hbm, xb.at[pl.ds(OWN, 8)], loc_sem.at[0])
    own_v = [pltpu.make_async_copy(v_hbm.at[:, pl.ds(i * CH, CH)], vb.at[OWN + i], loc_sem.at[1 + i])
             for i in range(8)]
    own_x.start()
    for c in own_v:
        c.start()
    barrier = pltpu.get_barrier_semaphore()
    for dev in (sib, left, right):
        pl.semaphore_signal(barrier, inc=1, device_id={"group": dev},
                            device_id_type=pl.DeviceIdType.MESH)
    y[...] = jnp.zeros_like(y)
    kb[...] = jnp.zeros_like(kb)
    ell = jnp.full((8, CH), ell_ref[0], jnp.float32)
    cst[0:8, :] = (2.0 * LOG2E) / (2.0 * ell * ell)
    cst[8:16, :] = jnp.log2(jnp.full((8, CH), s_ref[0], jnp.float32))
    own_x.wait()

    def target(slot, tile):
        xr[tile, 0:384, :] = xb[slot].T
        xr[tile, 384:512, :] = ext_rows(hb[slot], 3).astype(jnp.bfloat16)
        return 0

    def prep(slots):
        for s in slots:
            xe[s] = ext_rows(hb[s], 0).T.astype(jnp.bfloat16)

    def own_ext(i, _):
        hb[i] = half_norms(xb[i])
        return 0

    for c in own_v:
        c.wait()
    pl.semaphore_wait(barrier, 3)

    def rows_copy(src, dst, k, dev, count):
        return tuple(remote(buf.at[pl.ds(src, count)], buf.at[pl.ds(dst, count)], ss.at[k], rs.at[dst - SIB], dev)
                     for buf, ss, rs in ((hb, sh, rh), (xb, sx, rx), (vb, sv, rv)))

    def to_left(q, count):
        return rows_copy(OWN + (q + 4) % 8, LFT + q, 0, left, count)

    def to_right(q, count):
        return rows_copy(OWN + q, RGT + q, 1, right, count)

    def to_sib():
        return rows_copy(OWN, SIB, 2, sib, 8)

    def fwd(q, count):
        return rows_copy(LFT + q, LFT2 + q, 3, sib, count) + rows_copy(RGT + q, RGT2 + q, 4, sib, count)

    def all_sent():
        for k, (s, d, dev) in enumerate(((OWN, LFT, left), (OWN, RGT, right), (OWN, SIB, sib),
                                         (LFT, LFT2, sib), (RGT, RGT2, sib))):
            for c in rows_copy(s, d, k, dev, 8):
                c.wait_send()

    def partial_copies():
        return (remote(y.at[pl.ds(8, 4)], pin.at[pl.ds(0, 4)], ps.at[0], pr.at[0], left),
                remote(y.at[pl.ds(12, 4)], pin.at[pl.ds(4, 4)], ps.at[1], pr.at[1], right))

    first, rest = GROUPS[0], GROUPS[1:]
    early = [to_left(*first), to_right(*first), to_sib()]
    for c in early[0][1:] + early[1][1:] + early[2][1:]:
        c.start()
    lax.fori_loop(0, 2, lambda i, _: [own_ext(4 * i + k, 0) for k in range(4)][0], 0)
    lax.fori_loop(0, 2, lambda i, _: [target(OWN + 4 * i + k, 4 * i + k) for k in range(4)][0], 0)
    for copies in early:
        copies[0].start()
    for q, count in rest:
        for c in to_left(q, count) + to_right(q, count):
            c.start()

    def received(slot, count):
        for c in rows_copy(slot, slot, 0, sib, count):
            c.wait_recv()

    def arrive(q, count):
        received(LFT + q, count)
        received(RGT + q, count)
        for c in fwd(q, count):
            c.start()

    def arrive2(q, count):
        received(LFT2 + q, count)
        received(RGT2 + q, count)

    def dot(a, b):
        return jnp.dot(a, b, preferred_element_type=jnp.float32)

    def ext_lhs(slots):
        return jnp.concatenate([jnp.concatenate([xb[s], xe[s]], axis=1) for s in slots], axis=0)

    def k_tile(lhs, tile):
        e = jnp.minimum(dot(lhs, xr[tile]), 0.0) * cst[0:1, 0:1] + cst[8:9, 0:1]
        return jnp.exp2(e).astype(jnp.bfloat16)

    def kv(prev, src, i):
        g = i // 4
        lhs = jnp.concatenate([vb[prev[2 * g]], vb[prev[2 * g + 1]]], axis=1)
        y[prev[4] + i] += dot(lhs, src[i])

    def step(cur, prev, dst, src, halves=2, lag=2):
        for i in range(8):
            g = i // 4
            dst[i, 0:halves * CH, :] = k_tile(ext_lhs(cur[2 * g:2 * g + halves]), cur[4] + i)
            if src is not None and i >= lag:
                kv(prev, src, i - lag)
        if src is not None:
            for i in range(8 - lag, 8):
                kv(prev, src, i)

    def block(b, _):
        @pl.when(b == 2)
        def _():
            for c in to_sib():
                c.wait_recv()

        for table, event in ((ARRIVE, arrive), (ARRIVE2, arrive2)):
            for count, at in table.items():
                @pl.when(among(b, tuple(at)))
                def _(event=event, at=at, count=count):
                    event(at_block(b, at), count)

        @pl.when(b == SEND_BLOCK)
        def _():
            for c in partial_copies():
                c.start()

        @pl.when(b == 8)
        def _():
            lax.fori_loop(0, 2, lambda i, _: [target(base + 2 * i + k, tile + 2 * i + k)
                                              for base, tile in ((RGT, 8), (LFT, 12)) for k in range(2)][0], 0)

        t = 2 * b
        d0, d1, p = describe(t), describe(t + 1), describe(jnp.maximum(t - 1, 0))
        sl = [pick(b, 0, [row[k] for row in PREP]) for k in range(4)]
        prep(sl[0:2])
        step(d0, p, ka, kb)
        prep(sl[2:4])
        step(d1, d0, kb, ka)
        return 0

    lax.fori_loop(0, BLOCKS, block, 0)
    i32 = jnp.int32
    last = own_step(i32(LFT2 + 7), i32(RGT2 + 7))
    for i in range(8):
        kv(last, kb, i)
    all_sent()
    for c in partial_copies():
        c.wait()
    for i in range(8):
        out_ref[:, i * CH:(i + 1) * CH] = y[i] + pin[i]


def solution(mesh):
    n = mesh.shape["group"]
    row_spec = P(("tasks", "group"), None)

    def local_fn(x_loc, v_loc, lengthscale, outscale):
        rows, feat = x_loc.shape
        rhs = v_loc.shape[1]
        nc = rows // CH
        bf = jnp.bfloat16
        dma = pltpu.SemaphoreType.DMA
        out = pl.pallas_call(
            functools.partial(kernel, n),
            out_shape=pltpu.VMEM((rhs, rows), jnp.float32),
            in_specs=[pl.BlockSpec(memory_space=pl.ANY), pl.BlockSpec(memory_space=pl.ANY),
                      pl.BlockSpec(memory_space=pltpu.SMEM), pl.BlockSpec(memory_space=pltpu.SMEM)],
            out_specs=pl.BlockSpec(memory_space=pltpu.VMEM),
            scratch_shapes=[
                pltpu.VMEM((6 * nc, CH, feat), bf),
                pltpu.VMEM((6 * nc, rhs, CH), bf),
                pltpu.VMEM((6 * nc, 1, CH), jnp.float32),
                pltpu.VMEM((6 * nc, CH, 128), bf),
                pltpu.VMEM((2 * nc, feat + 128, CH), bf),
                pltpu.VMEM((nc, 2 * CH, CH), bf),
                pltpu.VMEM((nc, 2 * CH, CH), bf),
                pltpu.VMEM((2 * nc, rhs, CH), jnp.float32),
                pltpu.VMEM((nc, rhs, CH), jnp.float32),
                pltpu.VMEM((16, CH), jnp.float32),
                dma((9,)), dma((5,)), dma((5,)), dma((5,)), dma((5 * nc,)), dma((5 * nc,)), dma((5 * nc,)),
                dma((2,)), dma((2,)),
            ],
            compiler_params=pltpu.CompilerParams(
                collective_id=0, has_side_effects=True, vmem_limit_bytes=56 * 2**20),
        )(x_loc.reshape(nc, CH, feat), v_loc.T, lengthscale, outscale)
        return out.T

    return jax.shard_map(local_fn, mesh=mesh, in_specs=(row_spec, row_spec, P(None), P(None)),
                         out_specs=row_spec, check_vma=False)
```
